32 devices in a mesh: node: 4 (over z), grp: 2 (over y), rep: 4 (over x, core).
Axes of the slice: x: 2, y: 2, z: 4, core: 2. Of those that a mesh axis runs over, the one named last changes fastest.
Arguments:
- tokens: bfloat16 [1024, 768], P(('node', 'grp'), 'rep'), may hold values from -6 to 6
- gates: float32 [1024, 2], P(('node', 'grp')), may hold values from 0.05 to 1
- expert_ids: int32 [1024, 2], P(('node', 'grp')), may hold values from 0 to 7, all different within a row; in each aligned block of 128 rows (0 to 127, 128 to 255, ...) at most 64 rows name the same one
- w_in: bfloat16 [8, 768, 1536], P(('node', 'grp'), None, 'rep'), may hold values from -0.21875 to 0.21875
- b_in: float32 [8, 1536], P(('node', 'grp'), 'rep'), may hold values from -3 to 3
- w_out: bfloat16 [8, 1536, 768], P(('node', 'grp'), 'rep'), may hold values from -0.15625 to 0.15625
- b_out: float32 [8, 768], P(('node', 'grp'), 'rep'), may hold values from -3 to 3
- cotangent: bfloat16 [1024, 768], P(('node', 'grp'), 'rep'), may hold values from -6 to 6
Outputs:
- mixed: bfloat16 [1024, 768], P(('node', 'grp'), 'rep')
- d_tokens: bfloat16 [1024, 768], P(('node', 'grp'), 'rep')
- d_gates: float32 [1024, 2], P(('node', 'grp'))
- d_w_in: float32 [8, 768, 1536], P(('node', 'grp'), None, 'rep')
- d_b_in: float32 [8, 1536], P(('node', 'grp'), 'rep')
- d_w_out: float32 [8, 1536, 768], P(('node', 'grp'), 'rep')
- d_b_out: float32 [8, 768], P(('node', 'grp'), 'rep')
The draws below stay inside these ranges and needn't reach their ends.
Inputs may be any that keep to these rules, and one draw needn't show every extreme that they name: `expert_ids`: each row names 2 different experts. Among the 128 rows of one device's aligned block no expert is named more than 64 times, and in some blocks one expert is named exactly 64 times.
All inputs are finite; a program needn't handle non-finite values.
Results may differ from the reference program's by a relative error of at most 0.0064.
Values may be sent and summed in bfloat16 or wider, within the bound.
No kernel may reach another device: no remote copies, remote signals or barrier semaphores. Data moves between devices by JAX's collectives and lax.ppermute only.
A program may use at most 64 MiB of HBM per device.

```python
import math
import jax
import jax.numpy as jnp
import numpy as np
from jax import lax

D = 768
HID = 1536
TOP = 2
TOK_DEV = 128
EXPERTS = 8
CAP = 64
TOKENS = 1024


def shard_levels(key, shape, pieces, smallest, high):
    loudness, own = 1.0, jax.random.fold_in(key, 6)
    for axis_at, shards_of in pieces:
        draws = jnp.exp(jax.random.uniform(jax.random.fold_in(own, axis_at), (shards_of,), jnp.float32, smallest / len(pieces), high / len(pieces)))
        loudness = loudness * jnp.repeat(draws, shape[axis_at] // shards_of).reshape([-1 if axis == axis_at else 1 for axis in range(len(shape))])
    return loudness


def deal_out(own_key, own, number, rows, number_of, top, reach, skew):
    ranking = jax.random.permutation(own_key, number_of)
    crowded, usual = load_shares(number_of, rows * top, reach, skew, True), load_shares(number_of, rows * top, reach, skew, False)
    places = jnp.arange(number_of)

    def named(lengths, offset_by):
        used = int((lengths > 0).sum())
        fixed = max(1, used // 4)
        shifted = fixed + (places - fixed + offset_by * (used - fixed)) % max(1, number_of - fixed)
        return jnp.zeros((number_of,), jnp.int32).at[ranking[jnp.where(places < fixed, places, shifted)]].set(jnp.asarray(lengths, jnp.int32))

    lengths = jnp.where(number % 4 == 0, named(crowded, number // 4), named(usual, number - number // 4 - 1))
    mixed = jax.random.permutation(jax.random.fold_in(own, 3), number_of)
    giver, sink = mixed[0:number_of // 2 * 2:2], mixed[1:number_of // 2 * 2:2]
    slack = jnp.minimum(lengths[giver] - 1, reach - lengths[sink]) // 2
    slack = jnp.where((giver == ranking[0]) | (sink == ranking[0]) | (lengths[sink] == 0), 0, jnp.maximum(slack, 0))
    shifted = jax.random.randint(jax.random.fold_in(own, 4), (number_of // 2,), 0, 1 << 20) % (slack + 1)
    lengths = lengths.at[giver].add(-shifted).at[sink].add(shifted)
    items = jnp.searchsorted(jnp.cumsum(lengths), jnp.arange(rows * top), side="right").astype(jnp.int32)
    grid = items.reshape(top, rows).T
    grid = grid[jax.random.permutation(jax.random.fold_in(own, 1), rows)]
    offset_by = jax.random.randint(jax.random.fold_in(own, 2), (rows, 1), 0, top)
    return jnp.take_along_axis(grid, (jnp.arange(top)[None, :] + offset_by) % top, axis=1)


def load_shares(count, total, limit, slope, full):
    weights = [(1 << 20) // math.isqrt(rank ** slope) + 1 for rank in range(1, count + 1)]
    largest = limit if full else min(limit, max(-(-total // count), total * weights[0] // sum(weights)))
    least = 1 if total - largest >= count - 1 else 0
    holding, spare = [largest] + [least] * (count - 1), total - largest - least * (count - 1)
    while spare > 0:
        free = [i for i in range(1, count) if holding[i] < largest] or [i for i in range(1, count) if holding[i] < limit]
        pool, budget = sum([weights[i] for i in free]), spare
        for i in free:
            addition = min(limit - holding[i], max(1, budget * weights[i] // pool), spare)
            holding[i] = holding[i] + addition
            spare = spare - addition
    return np.array(holding)


def scatter_about(own_key, extent, scale, most, pieces=(), held_as=jnp.bfloat16):
    array = scale * jax.random.normal(own_key, extent, jnp.float32)
    if pieces:
        array = array * shard_levels(own_key, extent, pieces, -0.22, 0.18)
    return jnp.clip(array, -most, most).astype(held_as)


def setup_inputs(seed: int = 0) -> dict:
    splits = jax.random.split(jax.random.key(seed), 9)
    tokens = scatter_about(splits[0], (TOKENS, D), 1.0, 6.0, ((0, 8), (1, 4)))
    gates = jnp.clip(jnp.exp(math.log(1.0) - 2.9957323 * jax.random.uniform(splits[1], (TOKENS, TOP), jnp.float32) ** shard_levels(splits[1], (TOKENS, TOP), ((0, 8),), -0.2, 0.2)), 0.05, 1.0)
    expert_ids_keys = jax.random.split(jax.random.fold_in(splits[2], 1), TOKENS // TOK_DEV)
    expert_ids_turns = jax.random.permutation(jax.random.fold_in(splits[2], 3), TOKENS // TOK_DEV)
    expert_ids = jax.vmap(lambda own, number: deal_out(jax.random.fold_in(splits[2], 2), own, number, TOK_DEV, EXPERTS, TOP, CAP, 2))(expert_ids_keys, expert_ids_turns).reshape((TOKENS, TOP))
    w_in = scatter_about(splits[3], (EXPERTS, D, HID), D ** -0.5, 0.21875, ((0, 8), (2, 4)))
    b_in = scatter_about(splits[4], (EXPERTS, HID), 0.5, 3.0, ((0, 8), (1, 4)), jnp.float32)
    w_out = scatter_about(splits[5], (EXPERTS, HID, D), HID ** -0.5, 0.15625, ((0, 8), (1, 4)))
    b_out = scatter_about(splits[6], (EXPERTS, D), 0.5, 3.0, ((0, 8), (1, 4)), jnp.float32)
    cotangent = scatter_about(splits[7], (TOKENS, D), 1.0, 6.0, ((0, 8), (1, 4)))
    return dict(tokens=tokens, gates=gates, expert_ids=expert_ids, w_in=w_in, b_in=b_in, w_out=w_out, b_out=b_out, cotangent=cotangent)


def slot_ranks(row_ids):
    position = jnp.arange(row_ids.shape[0], dtype=jnp.int32)
    matches = (row_ids[:, None] == row_ids[None, :]) & (position[None, :] < position[:, None])
    return lax.optimization_barrier(jnp.sum(matches.astype(jnp.int32), axis=1)).astype(jnp.int32)

def pick_rows(source_rows, index, filled):
    safe_index = jnp.where(filled, index, 0).astype(jnp.int32)
    return jnp.where(filled[:, None], source_rows[safe_index], 0).astype(source_rows.dtype)

def contract_first(left, right):
    return lax.dot_general(left, right, (((0,), (0,)), ((), ())), preferred_element_type=jnp.float32)

def contract_last(left, right):
    return lax.dot_general(left, right, (((1,), (1,)), ((), ())), preferred_element_type=jnp.float32)

def reference(tokens, gates, expert_ids, w_in, b_in, w_out, b_out, cotangent):
    assigned = TOK_DEV * TOP
    blocks = expert_ids.reshape(EXPERTS, assigned).astype(jnp.int32)
    slot_rank = jax.vmap(slot_ranks)(blocks)
    source = jnp.arange(EXPERTS, dtype=jnp.int32)[:, None]
    target = ((blocks * EXPERTS + source) * CAP + slot_rank).reshape(-1).astype(jnp.int32)
    total_slots = EXPERTS * EXPERTS * CAP
    owner = jnp.full((total_slots,), -1, jnp.int32).at[target].set(jnp.arange(TOKENS * TOP, dtype=jnp.int32))
    owner = owner.reshape(EXPERTS, EXPERTS * CAP)

    def expert_forward(operands):
        slot_owner, w_first, bias_first, w_second, bias_second = operands
        filled = slot_owner >= 0
        expert_rows = pick_rows(tokens, slot_owner // TOP, filled)
        pre_act = jnp.dot(expert_rows, w_first, preferred_element_type=jnp.float32) + bias_first
        hidden = jax.nn.gelu(pre_act).astype(jnp.bfloat16)
        return (jnp.dot(hidden, w_second, preferred_element_type=jnp.float32) + bias_second).astype(jnp.bfloat16)
    expert_out = lax.map(expert_forward, (owner, w_in, b_in, w_out, b_out)).reshape(total_slots, D)
    per_assign = expert_out[target].reshape(TOKENS, TOP, D).astype(jnp.float32)
    mixed = lax.optimization_barrier(jnp.sum(gates[:, :, None] * per_assign, axis=1)).astype(jnp.bfloat16)
    cot_wide = cotangent.astype(jnp.float32)
    d_gates = lax.optimization_barrier(jnp.sum(cot_wide[:, None, :] * per_assign, axis=2))
    d_out = (gates[:, :, None] * cot_wide[:, None, :]).astype(jnp.bfloat16).reshape(TOKENS * TOP, D)

    def expert_backward(operands):
        slot_owner, w_first, bias_first, w_second = operands
        filled = slot_owner >= 0
        expert_rows = pick_rows(tokens, slot_owner // TOP, filled)
        grad_rows = pick_rows(d_out, slot_owner, filled)
        pre_act = jnp.dot(expert_rows, w_first, preferred_element_type=jnp.float32) + bias_first
        hidden = jax.nn.gelu(pre_act).astype(jnp.bfloat16)
        grad_bias_out = lax.optimization_barrier(jnp.sum(grad_rows.astype(jnp.float32), axis=0))
        grad_w_out = contract_first(hidden, grad_rows)
        d_hidden = contract_last(grad_rows, w_second)
        _, pull_back = jax.vjp(jax.nn.gelu, pre_act)
        d_pre = pull_back(d_hidden)[0].astype(jnp.bfloat16)
        grad_bias_in = lax.optimization_barrier(jnp.sum(d_pre.astype(jnp.float32), axis=0))
        grad_w_in = contract_first(expert_rows, d_pre)
        d_row = contract_last(d_pre, w_first).astype(jnp.bfloat16)
        return (d_row, grad_w_in, grad_bias_in, grad_w_out, grad_bias_out)
    d_row, d_w_in, d_b_in, d_w_out, d_b_out = lax.map(expert_backward, (owner, w_in, b_in, w_out))
    row_grads = d_row.reshape(total_slots, D)[target].reshape(TOKENS, TOP, D).astype(jnp.float32)
    d_tokens = lax.optimization_barrier(jnp.sum(row_grads, axis=1)).astype(jnp.bfloat16)
    return (mixed, d_tokens, d_gates, d_w_in, d_b_in, d_w_out, d_b_out)
```

```python
import jax
import jax.numpy as jnp
from jax import lax
from jax.sharding import PartitionSpec as P

GROUP = ("node", "grp")
EVERY = ("node", "grp", "rep")


def dot(left, right, contract):
    return lax.dot_general(
        left, right, ((contract[0], contract[1]), ((), ())), preferred_element_type=jnp.float32
    )


def per_device(tokens, gates, expert_ids, w_in, b_in, w_out, b_out, cotangent):
    bf16, f32 = jnp.bfloat16, jnp.float32
    n_experts = lax.axis_size(GROUP)
    n_rep = lax.axis_size("rep")
    tok_rows, quarter = tokens.shape
    top_k = expert_ids.shape[1]
    half = 2 * quarter
    capacity = max(2, 2 * tok_rows * top_k // n_experts)
    pieces = n_experts // 2
    rows = pieces * capacity
    block = lax.axis_index(GROUP)
    rep = lax.axis_index("rep")
    core = rep % 2
    first_half = rep // 2
    first_core = core == 0

    def swap(array, bit):
        return lax.ppermute(array, "rep", [(r, r ^ bit) for r in range(n_rep)])

    def routes(step):
        pairs = []
        for source in range(n_experts):
            for r in range(n_rep):
                other = source ^ (2 * step + r % 2)
                if other != source:
                    pairs.append((source * n_rep + r, other * n_rep + r))
        return pairs

    def exchange(buffer):
        arrived = []
        for step in range(pieces):
            piece = buffer[step]
            moved = lax.ppermute(piece, EVERY, routes(step))
            if step == 0:
                moved = jnp.where(first_core, piece, moved)
            arrived.append(moved)
        return jnp.concatenate(arrived, axis=0)

    def in_order(mine, theirs, mine_first, axis):
        return jnp.where(
            mine_first,
            jnp.concatenate([mine, theirs], axis=axis),
            jnp.concatenate([theirs, mine], axis=axis),
        )

    local = jnp.concatenate([tokens, cotangent], axis=1)
    nearby = swap(local, 1)
    tok_half = in_order(tokens, nearby[:, :quarter], first_core, 1)
    cot_half = in_order(cotangent, nearby[:, quarter:], first_core, 1)

    flat_ids = expert_ids.reshape(tok_rows * top_k)
    position = jnp.arange(tok_rows * top_k, dtype=jnp.int32)
    matches = (flat_ids[:, None] == flat_ids[None, :]) & (position[None, :] < position[:, None])
    slot_rank = jnp.sum(matches.astype(jnp.int32), axis=1).reshape(tok_rows, top_k)
    relative = expert_ids ^ block
    slot = jnp.where(relative % 2 == core, (relative // 2) * capacity + slot_rank, -1)
    slot_numbers = jnp.arange(rows, dtype=jnp.int32)[:, None]
    placing = [(slot_numbers == slot[None, :, k]).astype(bf16) for k in range(top_k)]
    placing_any = sum(placing)
    placing_each = jnp.concatenate(placing, axis=1)
    cot_wide = cot_half.astype(f32)
    d_out = jnp.concatenate([(gates[:, k : k + 1] * cot_wide).astype(bf16) for k in range(top_k)], axis=0)
    out_tok = dot(placing_any, tok_half, ((1,), (0,))).astype(bf16)
    out_grad = dot(placing_each, d_out, ((1,), (0,))).astype(bf16)
    outbound = jnp.concatenate([out_tok, out_grad], axis=1).reshape(pieces, capacity, 2 * half)

    own_a = exchange(outbound)
    own_b = swap(own_a, 2)
    far_a = swap(own_a, 1)
    far_b = swap(own_b, 1)
    all_a = jnp.concatenate([own_a, far_a], axis=0)
    all_b = jnp.concatenate([own_b, far_b], axis=0)
    tok_a, grad_a = all_a[:, :half], all_a[:, half:]
    tok_b, grad_b = all_b[:, :half], all_b[:, half:]

    offset_a = first_half * half
    offset_b = half - offset_a
    w1 = w_in[0]
    w2 = w_out[0]
    w1_a = lax.dynamic_slice_in_dim(w1, offset_a, half, 0)
    w1_b = lax.dynamic_slice_in_dim(w1, offset_b, half, 0)
    w2_a = lax.dynamic_slice_in_dim(w2, offset_a, half, 1)
    w2_b = lax.dynamic_slice_in_dim(w2, offset_b, half, 1)
    bias = lax.dynamic_update_slice_in_dim(jnp.zeros((2 * half,), f32), b_out[0], rep * quarter, 0)
    bias_a = lax.dynamic_slice_in_dim(bias, offset_a, half, 0)
    bias_b = lax.dynamic_slice_in_dim(bias, offset_b, half, 0)

    pre = dot(tok_a, w1_a, ((1,), (0,))) + dot(tok_b, w1_b, ((1,), (0,))) + b_in[0]
    hidden_wide, pull_back = jax.vjp(jax.nn.gelu, pre)
    hidden = hidden_wide.astype(bf16)
    y_a = dot(hidden, w2_a, ((1,), (0,))) + bias_a
    y_b = dot(hidden, w2_b, ((1,), (0,))) + bias_b
    d_hidden = dot(grad_a, w2_a, ((1,), (1,))) + dot(grad_b, w2_b, ((1,), (1,)))
    d_pre = pull_back(d_hidden)[0].astype(bf16)
    r_a = dot(d_pre, w1_a, ((1,), (1,)))
    r_b = dot(d_pre, w1_b, ((1,), (1,)))

    partial_a = jnp.concatenate([y_a, r_a], axis=1)
    partial_b = jnp.concatenate([y_b, r_b], axis=1)
    sum_b = partial_b[:rows] + swap(partial_b[rows:].astype(bf16), 1)
    sum_a = partial_a[:rows] + swap(partial_a[rows:].astype(bf16), 1)
    total = (sum_a + swap(sum_b.astype(bf16), 2)).astype(bf16)

    returned = exchange(total.reshape(pieces, capacity, 2 * half))
    per_k = [dot(placing[k], returned[:, :half], ((0,), (0,))) for k in range(top_k)]
    row_grads = dot(placing_any, returned[:, half:], ((0,), (0,)))
    mixed_half = sum(gates[:, k : k + 1] * per_k[k] for k in range(top_k))
    keep = lambda a: jnp.where(first_core, a[:, :quarter], a[:, quarter:])
    give = lambda a: jnp.where(first_core, a[:, quarter:], a[:, :quarter])
    received = swap(
        jnp.concatenate([give(mixed_half), give(row_grads)], axis=1).astype(bf16), 1
    )
    mixed = (keep(mixed_half) + received[:, :quarter]).astype(bf16)
    d_tokens = (keep(row_grads) + received[:, quarter:]).astype(bf16)
    gate_terms = jnp.stack([jnp.sum(cot_wide * per_k[k], axis=1) for k in range(top_k)])
    d_gates = (gate_terms + swap(gate_terms, 1)) + (swap(gate_terms, 2) + swap(gate_terms, 3))

    dw1 = in_order(
        dot(tok_a, d_pre, ((0,), (0,))), dot(tok_b, d_pre, ((0,), (0,))), first_half == 0, 0
    )
    dw2 = in_order(
        dot(hidden, grad_a, ((0,), (0,))), dot(hidden, grad_b, ((0,), (0,))), first_half == 0, 1
    )
    db1 = jnp.sum(d_pre.astype(f32), axis=0)
    db2 = in_order(
        jnp.sum(grad_a.astype(f32), axis=0), jnp.sum(grad_b.astype(f32), axis=0), first_half == 0, 0
    )
    db2 = lax.dynamic_slice_in_dim(db2, rep * quarter, quarter, 0)
    return mixed, d_tokens, d_gates.T, dw1[None], db1[None], dw2[None], db2[None]


def solution(mesh):
    split, inner = P(GROUP, "rep"), P(GROUP, None, "rep")
    whole, outer = P(GROUP, None), P(GROUP, "rep", None)
    return jax.shard_map(
        per_device,
        mesh=mesh,
        in_specs=(split, whole, whole, inner, split, outer, split, split),
        out_specs=(split, split, whole, inner, split, outer, split),
        check_vma=False,
    )
```

```python
import functools

import jax
import jax.numpy as jnp
from jax import lax
from jax.experimental import pallas as pl
from jax.experimental.pallas import tpu as pltpu
from jax.sharding import PartitionSpec as P

GROUP = ("node", "grp")
EVERY = ("node", "grp", "rep")
BF16, F32 = jnp.bfloat16, jnp.float32
ROOT_2_OVER_PI = 0.7978845608028654


def dot(left, right, left_dim, right_dim):
    return lax.dot_general(
        left, right, (((left_dim,), (right_dim,)), ((), ())), preferred_element_type=F32
    )


def like(shape, dtype):
    return jax.ShapeDtypeStruct(shape, dtype)


def call(kernel, arrays, outs, flops, name, mib, source=pltpu.VMEM, scratch=()):
    spec = pl.BlockSpec(memory_space=pltpu.VMEM)
    moved = sum(a.size * a.dtype.itemsize for a in (*arrays, *outs))
    return pl.pallas_call(
        kernel,
        out_shape=outs,
        in_specs=[pl.BlockSpec(memory_space=source)] * len(arrays),
        out_specs=[spec] * len(outs),
        scratch_shapes=list(scratch),
        cost_estimate=pl.CostEstimate(flops=flops, bytes_accessed=moved, transcendentals=0),
        compiler_params=pltpu.CompilerParams(vmem_limit_bytes=mib << 20),
        name=name,
    )(*arrays)


def core():
    return lax.rem(lax.axis_index("rep"), 2)


def spans(half):
    side = lax.div(lax.axis_index("rep"), 2)
    near = pl.multiple_of(side * half, 128)
    far = pl.multiple_of((1 - side) * half, 128)
    return pl.ds(near, half), pl.ds(far, half)


def route_kernel(capacity, ids_hbm, gates_hbm, tok_hbm, cot_hbm, placing, local, gates, ids, sems):
    quarter = tok_hbm.shape[0]
    reads = [
        pltpu.make_async_copy(source, target, sems.at[n])
        for n, (source, target) in enumerate(
            (
                (ids_hbm, ids),
                (tok_hbm, local.at[:quarter]),
                (cot_hbm, local.at[quarter:]),
                (gates_hbm, gates),
            )
        )
    ]
    for read in reads:
        read.start()
    top_k, rows, tokens = placing.shape
    slot = lax.broadcasted_iota(jnp.int32, (rows, tokens), 0)
    expert = lax.axis_index(GROUP) ^ (2 * lax.div(slot, capacity) + core())
    wanted = lax.rem(slot, capacity).astype(F32)
    earlier = lax.broadcasted_iota(jnp.int32, (tokens, tokens), 0) < lax.broadcasted_iota(
        jnp.int32, (tokens, tokens), 1
    )
    reads[0].wait()
    named = [ids[k : k + 1, :] == expert for k in range(top_k)]
    some = functools.reduce(jnp.logical_or, named)
    rank = dot(some.astype(F32).astype(BF16), earlier.astype(F32).astype(BF16), 1, 0)
    for k in range(top_k):
        placing[k] = jnp.where(named[k] & (rank == wanted), 1.0, 0.0).astype(BF16)
    for read in reads[1:]:
        read.wait()


def any_choice(placing):
    return functools.reduce(jnp.add, [placing[k] for k in range(placing.shape[0])])


def both_cores(mine, near):
    first = core() == 0
    return jnp.concatenate([jnp.where(first, mine, near), jnp.where(first, near, mine)], axis=0)


def send_kernel(capacity, placing, gates, local, near, out, cot_half):
    quarter = local.shape[0] // 2
    pieces = out.shape[0]
    cot = both_cores(local[quarter:], near[quarter:])
    cot_half[...] = cot
    wide = cot.astype(F32)
    moved_tokens = dot(any_choice(placing), both_cores(local[:quarter], near[:quarter]), 1, 1)
    moved_grads = None
    for k in range(placing.shape[0]):
        part = dot(placing[k], (gates[k : k + 1, :] * wide).astype(BF16), 1, 1)
        moved_grads = part if moved_grads is None else moved_grads + part
    for kind, moved in enumerate((moved_tokens, moved_grads)):
        out[:, kind] = moved.reshape(pieces, capacity, moved.shape[1]).astype(BF16)


def expert_kernel(
    own_a, own_b, far_a, far_b, w1, b1, w2, bias,
    hidden, d_pre, sum_own_a, sum_own_b, sum_far_a, sum_far_b,
):
    half = own_a.shape[2]
    near, far = spans(half)
    outs = ((sum_own_a, sum_own_b), (sum_far_a, sum_far_b))
    for side, (a, b) in ((1, (far_a, far_b)), (0, (own_a, own_b))):
        pre = dot(a[0], w1[near, :], 1, 0) + dot(b[0], w1[far, :], 1, 0) + b1[...]
        square = pre * pre
        bent = jnp.tanh(ROOT_2_OVER_PI * pre * (1.0 + 0.044715 * square))
        up = 0.5 * (1.0 + bent)
        slope = up + 0.5 * pre * (1.0 - bent * bent) * (
            ROOT_2_OVER_PI * (1.0 + 3 * 0.044715 * square)
        )
        active = (pre * up).astype(BF16)
        hidden[side] = active
        d_hidden = dot(a[1], w2[:, near], 1, 1) + dot(b[1], w2[:, far], 1, 1)
        d_in = (d_hidden * slope).astype(BF16)
        d_pre[side] = d_in
        for ref, span in zip(reversed(outs[side]), (far, near)):
            ref[:, :half] = (dot(active, w2[:, span], 1, 0) + bias[:, span]).astype(ref.dtype)
            ref[:, half:] = dot(d_in, w1[span, :], 1, 1).astype(ref.dtype)


def weights_kernel(count, *refs):
    batches = [refs[4 * n : 4 * n + 4] for n in range(count)]
    hiddens, d_pres = refs[4 * count : 5 * count], refs[5 * count : 6 * count]
    dw1, db1, dw2, db2 = refs[6 * count :]
    near, far = spans(batches[0][0].shape[2])

    def stack(kind, letter):
        parts = [batch[side + letter][kind] for batch in batches for side in (0, 2)]
        return jnp.concatenate(parts, axis=0)

    d_pre = jnp.concatenate([ref[side] for ref in d_pres for side in (0, 1)], axis=0)
    hidden = jnp.concatenate([ref[side] for ref in hiddens for side in (0, 1)], axis=0)
    for letter, span in enumerate((near, far)):
        grads = stack(1, letter)
        dw1[0, span, :] = dot(stack(0, letter), d_pre, 0, 0)
        dw2[0, :, span] = dot(hidden, grads, 0, 0)
        db2[:, span] = jnp.sum(grads.astype(F32), axis=0, keepdims=True)
    db1[...] = jnp.sum(d_pre.astype(F32), axis=0, keepdims=True)


def unplace_kernel(back, placing, gates, cot_half, keep, give, terms):
    half = cot_half.shape[0]
    quarter = half // 2
    cot = cot_half[...].astype(F32)
    mixed = None
    for k in range(placing.shape[0]):
        rows = dot(back[:, :half], placing[k], 0, 0)
        part = gates[k : k + 1, :] * rows
        mixed = part if mixed is None else mixed + part
        terms[k : k + 1, :] = jnp.sum(cot * rows, axis=0, keepdims=True)
    first = core() == 0
    for kind, whole in enumerate((mixed, dot(back[:, half:], any_choice(placing), 0, 0))):
        span = slice(kind * quarter, (kind + 1) * quarter)
        keep[span] = jnp.where(first, whole[:quarter], whole[quarter:])
        give[span] = jnp.where(first, whole[quarter:], whole[:quarter]).astype(BF16)


def finish_kernel(keep, near, terms, by_core, by_chip, by_both, mixed, d_tokens, d_gates):
    quarter = mixed.shape[0]
    mixed[...] = (keep[:quarter] + near[:quarter]).astype(BF16)
    d_tokens[...] = (keep[quarter:] + near[quarter:]).astype(BF16)
    d_gates[...] = (terms[...] + by_core[...]) + (by_chip[...] + by_both[...])


def per_device(tokens, gates, expert_ids, w_in, b_in, w_out, b_out, cotangent):
    n_experts = lax.axis_size(GROUP)
    n_rep = lax.axis_size("rep")
    tok_rows, quarter = tokens.shape
    top_k = expert_ids.shape[1]
    half = 2 * quarter
    units = w_in.shape[2]
    capacity = max(2, 2 * tok_rows * top_k // n_experts)
    pieces = n_experts // 2
    rows = pieces * capacity
    block = lax.axis_index(GROUP)
    rep = lax.axis_index("rep")
    def swap(array, bit):
        return lax.ppermute(array, "rep", [(r, r ^ bit) for r in range(n_rep)])

    def exchange(piece, step):
        pairs = []
        for source in range(n_experts):
            for r in range(n_rep):
                other = source ^ (2 * step + r % 2)
                pairs.append((source * n_rep + r, other * n_rep + r))
        return lax.ppermute(piece, EVERY, pairs)

    placing, local, gates_t = call(
        functools.partial(route_kernel, capacity),
        [expert_ids.T, gates.T, tokens.T, cotangent.T],
        [
            like((top_k, rows, tok_rows), BF16), like((half, tok_rows), BF16),
            like((top_k, tok_rows), F32),
        ],
        2 * rows * tok_rows * tok_rows, "route", 4, pltpu.HBM,
        [pltpu.VMEM((top_k, tok_rows), jnp.int32), pltpu.SemaphoreType.DMA((4,))],
    )
    moving = 2 * rows * tok_rows * half
    outbound, cot_half = call(
        functools.partial(send_kernel, capacity), [placing, gates_t, local, swap(local, 1)],
        [like((pieces, 2, capacity, half), BF16), like((half, tok_rows), BF16)],
        3 * moving, "send", 8,
    )

    w1, w2 = w_in[0], w_out[0]
    bias = lax.dynamic_update_slice_in_dim(jnp.zeros((1, 2 * half), F32), b_out, rep * quarter, 1)
    halves = [range(pieces // 2), range(pieces // 2, pieces)]
    batches, hiddens, d_pres, backs = [], [], [], []
    arrived = [exchange(outbound[step], step) for step in range(pieces)]
    for steps in halves:
        count = len(steps) * capacity
        own_a = jnp.concatenate([arrived[step] for step in steps], axis=1)
        own_b = swap(own_a, 2)
        far_a = swap(own_a, 1)
        if hiddens:
            own_b, hiddens[-1] = lax.optimization_barrier((own_b, hiddens[-1]))
        batch = [own_a, own_b, far_a, swap(own_b, 1)]
        hidden, d_pre, sum_own_a, sum_own_b, sum_far_a, sum_far_b = call(
            expert_kernel, [*batch, w1, b_in, w2, bias],
            [
                *[like((2, count, units), BF16)] * 2, *[like((count, 2 * half), F32)] * 2,
                *[like((count, 2 * half), BF16)] * 2,
            ],
            8 * 2 * count * 2 * half * units, "expert", 16,
        )
        batches.extend(batch)
        hiddens.append(hidden)
        d_pres.append(d_pre)
        sum_b = (sum_own_b + swap(sum_far_b, 1)).astype(BF16)
        total = (sum_own_a + swap(sum_far_a, 1) + swap(sum_b, 2)).astype(BF16)
        for place, step in enumerate(steps):
            backs.append(exchange(total[place * capacity : (place + 1) * capacity], step))
    dw1, db1, dw2, db2 = call(
        functools.partial(weights_kernel, len(halves)), [*batches, *hiddens, *d_pres],
        [
            like((1, 2 * half, units), F32), like((1, units), F32),
            like((1, units, 2 * half), F32), like((1, 2 * half), F32),
        ],
        4 * 2 * rows * 2 * half * units, "weights", 16,
    )

    keep, give, terms = call(
        unplace_kernel, [jnp.concatenate(backs, axis=0), placing, gates_t, cot_half],
        [
            like((half, tok_rows), F32), like((half, tok_rows), BF16),
            like((top_k, tok_rows), F32),
        ],
        3 * moving, "unplace", 8,
    )
    mixed, d_tokens, d_gates = call(
        finish_kernel,
        [keep, swap(give, 1), terms, swap(terms, 1), swap(terms, 2), swap(terms, 3)],
        [*[like((quarter, tok_rows), BF16)] * 2, like((top_k, tok_rows), F32)],
        half * tok_rows, "finish", 4,
    )
    db2 = lax.dynamic_slice_in_dim(db2, rep * quarter, quarter, 1)
    return mixed.T, d_tokens.T, d_gates.T, dw1, db1, dw2, db2


def solution(mesh):
    split, inner = P(GROUP, "rep"), P(GROUP, None, "rep")
    whole, outer = P(GROUP, None), P(GROUP, "rep", None)
    return jax.shard_map(
        per_device,
        mesh=mesh,
        in_specs=(split, whole, whole, inner, split, outer, split, split),
        out_specs=(split, split, whole, inner, split, outer, split),
        check_vma=False,
    )
```
